32 devices in a mesh: groups: 2 (over x), pb: 8 (over z, y), ka: 2 (over core).
Axes of the slice: x: 2, y: 2, z: 4, core: 2. Of those that a mesh axis runs over, the one named last changes fastest.
Arguments:
- queries: bfloat16 [12288, 256], P(('groups', 'pb', 'ka')), parts along dimension 0, may hold values from -6 to 6
- keys: bfloat16 [12288, 256], P(('groups', 'pb', 'ka')), parts along dimension 0, may hold values from -6 to 6
- values: bfloat16 [12288, 256], P(('groups', 'pb', 'ka')), parts along dimension 0, may hold values from -96 to 96
- block_pairs: int32 [4, 8, 16, 9], P('groups', 'pb'), parts along dimension 0, may hold values from -1 to 17, as said below
Outputs:
- attended: bfloat16 [12288, 256], P(('groups', 'pb', 'ka')), parts along dimension 0
The draws below stay inside these ranges and needn't reach their ends.
There are 2 independent parts, one for each index of `groups`. The reference program is written for one: setup_inputs(seed, part) draws one part's arguments, and reference() takes and returns one part's arrays. A program takes and returns all parts, laid end to end along the dimension named above; each array names one. Nothing has to cross between parts.
Inputs may be any that keep to these rules, and one draw needn't show every extreme that they name: Each list block_pairs[h, p, s, :] holds 1 to 9 distinct codes (as defined in the reference program) followed by entries -1; in every draw some list holds 9 codes. Every query block's pair with the key block of the same tokens is kept for every head.
All inputs are finite; a program needn't handle non-finite values.
Results may differ from the reference program's by a relative error of at most 0.0085.
Values may be sent and summed in bfloat16 or wider, within the bound.
No kernel may reach another device: no remote copies, remote signals or barrier semaphores. Data moves between devices by JAX's collectives and lax.ppermute only.
A program may use at most 128 MiB of HBM per device.

```python
import jax
import jax.numpy as jnp
from jax import lax

HEAD = 128
HEADS = 2
BLOCK = 128
TOK_DEV = 384
MOST = 9
TOKENS = 6144
N_PB = 8
N_KA = 2


def base_field(key):
    field_shape = (TOKENS, HEADS * HEAD)
    matrix = jax.random.normal(jax.random.fold_in(key, 2), field_shape, jnp.float32)
    return jnp.clip(matrix, -6.0, 6.0)


def draw_queries(key, part):
    matrix = base_field(jax.random.fold_in(key, 11))
    return matrix.astype(jnp.bfloat16)


def draw_keys(key, part):
    matrix = base_field(jax.random.fold_in(key, 12))
    return matrix.astype(jnp.bfloat16)


def draw_block_pairs(key, part):
    shard_count = N_PB * N_KA
    shard_blocks = TOK_DEV // BLOCK
    grid_size = N_KA * shard_blocks * shard_blocks
    levels = jax.random.randint(jax.random.fold_in(key, 21), (HEADS, N_PB, 1, N_KA), 0, 3)
    levels = jnp.broadcast_to(levels, (HEADS, N_PB, N_PB, N_KA)).reshape(HEADS, N_PB, shard_count)
    counts = jax.random.randint(jax.random.fold_in(key, 22), (HEADS, N_PB, shard_count), 1, MOST // 2 + 1)
    counts = counts + levels * (MOST // 4)
    tile_ids = jnp.arange(N_PB)[:, None]
    shard_ids = jnp.arange(shard_count)[None, :]
    own_shard = shard_ids // N_KA == tile_ids
    counts = jnp.where(own_shard[None], jnp.maximum(counts, shard_blocks + 1), counts)
    flat_ids = jnp.arange(N_PB * shard_count).reshape(N_PB, shard_count)
    chosen = jax.random.randint(jax.random.fold_in(key, 23), (HEADS, 1, 1), 0, N_PB * shard_count)
    counts = jnp.minimum(jnp.where(flat_ids[None] == chosen, MOST, counts), MOST)
    places = jnp.arange(grid_size)
    query_local = places // shard_blocks
    key_local = places % shard_blocks
    diagonal = (shard_ids[:, :, None] == tile_ids[:, :, None] * N_KA + (query_local // shard_blocks)[None, None, :]) & (key_local == query_local % shard_blocks)[None, None, :]
    jitter = jax.random.randint(jax.random.fold_in(key, 24), (HEADS, N_PB, shard_count, grid_size), 0, 1 << 16)
    priority = jitter * 1024 + places + diagonal[None].astype(jnp.int32) * (1 << 28)
    ranked = jnp.argsort(-priority, axis=-1, stable=True)[..., :MOST]
    slot_ids = jnp.arange(MOST)
    return jnp.where(slot_ids < counts[..., None], ranked, -1).astype(jnp.int32)


def block_scale(key, extent, split, low, high):
    gain, own = 1.0, jax.random.fold_in(key, 6)
    for dim, blocks in split:
        draws = jnp.exp(jax.random.uniform(jax.random.fold_in(own, dim), (blocks,), jnp.float32, low / len(split), high / len(split)))
        gain = gain * jnp.repeat(draws, extent[dim] // blocks).reshape([-1 if axis == dim else 1 for axis in range(len(extent))])
    return gain


def scatter_about(stream_key, dims, width, reach, cuts=(), kind=jnp.bfloat16):
    result = width * jax.random.normal(stream_key, dims, jnp.float32)
    if cuts:
        result = result * block_scale(stream_key, dims, cuts, -0.22, 0.18)
    return jnp.clip(result, -reach, reach).astype(kind)


def setup_inputs(seed: int = 0, part: int = 0) -> dict:
    splits = jax.random.split(jax.random.key(seed), 5)
    part_splits = jax.random.split(jax.random.fold_in(splits[4], part), 5)
    return {
        "queries": draw_queries(jax.random.fold_in(jax.random.fold_in(splits[4], part), 71), part),
        "keys": draw_keys(jax.random.fold_in(jax.random.fold_in(splits[4], part), 71), part),
        "values": scatter_about(part_splits[2], (TOKENS, HEADS * HEAD), 16.0, 96.0, ((0, 16),)),
        "block_pairs": draw_block_pairs(jax.random.fold_in(jax.random.fold_in(splits[4], part), 71), part),
    }


NEGATIVE_FILL = -1.0e30


def tile_attention(queries, keys, values, block_pairs, head_index, tile_index):
    shard_blocks = TOK_DEV // BLOCK
    tile_rows = N_KA * TOK_DEV
    tile_blocks = N_KA * shard_blocks
    shard_count = N_PB * N_KA
    per_head = lax.dynamic_index_in_dim(block_pairs, head_index, 0, keepdims=False)
    pair_codes = lax.dynamic_index_in_dim(per_head, tile_index, 0, keepdims=False).reshape(-1)
    active = pair_codes >= 0
    clean = jnp.where(active, pair_codes, 0).astype(jnp.int32)
    query_block = (clean // shard_blocks).astype(jnp.int32)
    shard_of = jnp.arange(shard_count * MOST, dtype=jnp.int32) // MOST
    key_block = (shard_of * shard_blocks + clean % shard_blocks).astype(jnp.int32)
    column_start = (head_index * HEAD).astype(jnp.int32)
    row_start = (tile_index * tile_rows).astype(jnp.int32)
    query_tile = lax.dynamic_slice(queries, (row_start, column_start), (tile_rows, HEAD))
    key_cols = lax.dynamic_slice_in_dim(keys, column_start, HEAD, 1).reshape(TOKENS // BLOCK, BLOCK, HEAD)
    value_cols = lax.dynamic_slice_in_dim(values, column_start, HEAD, 1).reshape(TOKENS // BLOCK, BLOCK, HEAD)
    query_sel = query_tile.reshape(tile_blocks, BLOCK, HEAD)[query_block].astype(jnp.float32)
    key_sel = key_cols[key_block].astype(jnp.float32)
    value_sel = value_cols[key_block].astype(jnp.float32)
    scores = jnp.einsum("nqd,nkd->nqk", query_sel, key_sel, precision=lax.Precision.HIGHEST) * (HEAD ** -0.5)
    scores = jnp.where(active[:, None, None], scores, NEGATIVE_FILL)
    slot_max = scores.max(-1)
    is_kept_pair = (query_block[:, None] == jnp.arange(tile_blocks, dtype=jnp.int32)[None, :]) & active[:, None]
    peak = jnp.where(is_kept_pair[:, :, None], slot_max[:, None, :], NEGATIVE_FILL).max(0)
    slot_peak = peak[query_block]
    chances = jnp.where(active[:, None, None], jnp.exp(scores - slot_peak[:, :, None]), 0.0)
    pair_flag = is_kept_pair.astype(jnp.float32)
    total = jnp.einsum("nb,nq->bq", pair_flag, chances.sum(-1), precision=lax.Precision.HIGHEST)
    softmax_weight = lax.optimization_barrier(chances.astype(jnp.bfloat16)).astype(jnp.float32)
    partial_output = jnp.einsum("nqk,nkd->nqd", softmax_weight, value_sel, precision=lax.Precision.HIGHEST)
    running_output = jnp.einsum("vw,vhs->whs", pair_flag, partial_output, precision=lax.Precision.HIGHEST)
    return (running_output / total[:, :, None]).astype(jnp.bfloat16).reshape(tile_rows, HEAD)


def reference(queries, keys, values, block_pairs):
    head_numbers = jnp.repeat(jnp.arange(HEADS, dtype=jnp.int32), N_PB)
    tile_ids = jnp.tile(jnp.arange(N_PB, dtype=jnp.int32), HEADS)

    def one_tile(index_pair):
        return tile_attention(queries, keys, values, block_pairs, index_pair[0], index_pair[1])

    tile_outputs = lax.map(one_tile, (head_numbers, tile_ids))
    tile_outputs = tile_outputs.reshape(HEADS, N_PB, N_KA * TOK_DEV, HEAD).transpose(1, 2, 0, 3)
    return tile_outputs.reshape(TOKENS, HEADS * HEAD)
```

```python
import functools

import jax
import jax.numpy as jnp
from jax import lax
from jax.experimental import pallas as pl
from jax.experimental.pallas import tpu as pltpu
from jax.sharding import PartitionSpec as P

HEAD = 128
BLOCK = 128
LOG2_E = 1.4426950408889634
NEGATIVE_FILL = -1e30


def attend_kernel(first, last, count, slots_ref, bias_ref, q_ref, *refs):
    key_refs = refs[:count]
    value_refs = refs[count : 2 * count]
    refs = refs[2 * count :]
    if not first:
        accum_in, stat_in = refs[:2]
        refs = refs[2:]
    heads = q_ref.shape[1] // HEAD
    blocks = q_ref.shape[0] // BLOCK
    factor = HEAD**-0.5 * LOG2_E
    for head in range(heads):
        cols = slice(head * HEAD, (head + 1) * HEAD)
        for block in range(blocks):
            rows = slice(block * BLOCK, (block + 1) * BLOCK)
            query = q_ref[rows, cols]
            scores = []
            for slot in range(count):
                raw = lax.dot_general(
                    query,
                    key_refs[slot][:, cols],
                    (((1,), (1,)), ((), ())),
                    preferred_element_type=jnp.float32,
                )
                line = head * blocks + block
                scores.append(raw + bias_ref[slots_ref[slot], line : line + 1, :])
            peak = functools.reduce(jnp.maximum, scores).max(-1, keepdims=True)
            if not first:
                peak_old = stat_in[rows, head * HEAD : head * HEAD + 1]
                total_old = stat_in[rows, head * HEAD + 64 : head * HEAD + 65]
                peak = jnp.maximum(peak, peak_old)
                shrink = jnp.exp2((peak_old - peak) * factor)
            weights = [jnp.exp2((s - peak) * factor) for s in scores]
            total = functools.reduce(jnp.add, weights).sum(-1, keepdims=True)
            accum = functools.reduce(
                jnp.add,
                [
                    jnp.dot(
                        w.astype(jnp.bfloat16),
                        value_refs[slot][:, cols],
                        preferred_element_type=jnp.float32,
                    )
                    for slot, w in enumerate(weights)
                ],
            )
            if not first:
                total = total + shrink * total_old
                accum = accum + shrink * accum_in[rows, cols]
            if last:
                refs[0][rows, cols] = (accum / total).astype(jnp.bfloat16)
            else:
                refs[0][rows, cols] = accum
                lane = lax.broadcasted_iota(jnp.int32, (BLOCK, HEAD), 1)
                refs[1][rows, cols] = jnp.where(lane < 64, peak, total)


def attend(state, last, shard_ids, bias, queries, keys, values):
    first = state is None
    count = len(keys)
    rows, width = queries.shape
    vmem = pl.BlockSpec(memory_space=pltpu.VMEM)
    smem = pl.BlockSpec(memory_space=pltpu.SMEM)
    operands = [*keys, *values, *(() if first else state)]
    wide = jax.ShapeDtypeStruct((rows, width), jnp.float32)
    out = jax.ShapeDtypeStruct((rows, width), jnp.bfloat16) if last else (wide, wide)
    pairs = rows * keys[0].shape[0] * (width // HEAD) * count
    return pl.pallas_call(
        functools.partial(attend_kernel, first, last, count),
        out_shape=out,
        in_specs=[smem, vmem, vmem] + [vmem] * len(operands),
        out_specs=vmem if last else (vmem, vmem),
        compiler_params=pltpu.CompilerParams(vmem_limit_bytes=24 * 2**20),
        cost_estimate=pl.CostEstimate(
            flops=4 * pairs * HEAD, bytes_accessed=4 * rows * width * count, transcendentals=pairs
        ),
    )(jnp.stack(shard_ids).astype(jnp.int32), bias, queries, *operands)


def ring_order(count):
    return list(range(0, count, 2)) + list(range(count - 1 - count % 2, 0, -2))


def pair_bias(block_pairs, column, blocks):
    heads, shards, _ = block_pairs.shape
    wanted = jnp.arange(blocks * blocks, dtype=jnp.int32) + column * (blocks * blocks)
    kept = (block_pairs[..., None] == wanted).any(-2)
    bias = jnp.where(kept, 0.0, NEGATIVE_FILL).astype(jnp.float32)
    bias = bias.reshape(heads, shards, blocks, blocks).transpose(1, 0, 2, 3)
    return jnp.repeat(bias.reshape(shards, heads * blocks, blocks), BLOCK, axis=2)


def local(queries, keys, values, block_pairs):
    column = lax.axis_index("ka")
    chips = lax.axis_size("pb")
    columns = lax.axis_size("ka")
    blocks = keys.shape[0] // BLOCK
    order = ring_order(chips)
    ahead = [(order[i], order[(i + 1) % chips]) for i in range(chips)]
    behind = [(b, a) for a, b in ahead]
    swap = [(i, (i + 1) % columns) for i in range(columns)]
    me = lax.axis_index("pb")
    half = (chips + 1) // 2
    place = jnp.where(me % 2 == 0, me // 2, chips - 1 - me // 2)

    def chip_at(position):
        position = lax.rem(position + 2 * chips, chips)
        return jnp.where(position < half, 2 * position, 2 * (chips - 1 - position) + 1)

    bias = pair_bias(block_pairs[:, 0], column, blocks)

    def everywhere(chip, key_part, value_part):
        ids, key_list, value_list = [], [], []
        for turn in range(columns):
            ids.append(chip * columns + lax.rem(column - turn + columns, columns))
            key_list.append(key_part)
            value_list.append(value_part)
            if turn + 1 < columns:
                key_part = lax.ppermute(key_part, "ka", swap)
                value_part = lax.ppermute(value_part, "ka", swap)
        return ids, key_list, value_list

    def join(*groups):
        return [sum(parts, []) for parts in zip(*groups)]

    key_up = key_down = keys
    value_up = value_down = values
    state = attend(None, False, *_args(everywhere(me, keys, values), bias, queries))
    steps = (chips - 1) // 2
    for step in range(1, steps + 1):
        key_up = lax.ppermute(key_up, "pb", ahead)
        key_down = lax.ppermute(key_down, "pb", behind)
        value_up = lax.ppermute(value_up, "pb", ahead)
        value_down = lax.ppermute(value_down, "pb", behind)
        got = join(
            everywhere(chip_at(place - step), key_up, value_up),
            everywhere(chip_at(place + step), key_down, value_down),
        )
        last = step == steps and chips % 2 == 1
        state = attend(state, last, *_args(got, bias, queries))
    if chips % 2 == 0:
        key_up = lax.ppermute(key_up, "pb", ahead)
        value_down = lax.ppermute(value_down, "pb", behind)
        got = everywhere(chip_at(place + chips // 2), key_up, value_down)
        state = attend(state, True, *_args(got, bias, queries))
    return state


def _args(got, bias, queries):
    ids, key_list, value_list = got
    return ids, bias, queries, key_list, value_list


def solution(mesh):
    rows = P(("groups", "pb", "ka"), None)
    in_specs = (rows, rows, rows, P("groups", "pb", None, None))
    return jax.shard_map(local, mesh=mesh, in_specs=in_specs, out_specs=rows, check_vma=False)
```
